32 devices in a mesh: lat: 4 (over z), lon: 8 (over y, x, core).
Axes of the slice: x: 2, y: 2, z: 4, core: 2. Of those that a mesh axis runs over, the one named last changes fastest.
Arguments:
- poleward_flow: float32 [10, 4, 256, 1024], P(None, None, 'lat', 'lon'), may hold values from -16 to 16
- potential_warmth: float32 [10, 4, 256, 1024], P(None, None, 'lat', 'lon'), may hold values from -16 to 16
- water_profile_flag: int32 [256, 1024], P('lat', 'lon'), may hold values from 0 to 1
- floor_count: int32 [256, 1024], P('lat', 'lon'), may hold values from 0 to 4, as said below
- catchment_label_for_site: int32 [256, 1024], P('lat', 'lon'), may hold values from 0 to 9
Outputs:
- eddy_temp: float32 [4, 256, 1024], P(None, 'lat', 'lon')
- transport: float32 [4, 10, 4, 256], P(None, None, None, ('lat', 'lon'))
The draws below stay inside these ranges and needn't reach their ends.
Inputs may be any that keep to these rules, and one draw needn't show every extreme that they name: `floor_count`: land rows of zeros occur at some latitudes; elsewhere columns have 1 to 4 wet levels.
All inputs are finite; a program needn't handle non-finite values.
Results may differ from the reference program's by a relative error of at most 0.0003.
Values sent between devices are 32-bit elements; how exact they have to be, the bound alone decides.
A program may use at most 64 MiB of HBM per device.

```python
import math
import jax
import jax.numpy as jnp
from jax import lax

SNAPSHOT_TIMES = 10
LAYERS = 4
BASINS = 10
MERIDIAN_POINTS = 256
LONGITUDE_SLOTS = 1024


def ocean_fields(key):
    generator_keys = jax.random.split(jax.random.fold_in(key, 11), 10)
    along_latitude_flow = jax.random.normal(generator_keys[0], (1, LAYERS, MERIDIAN_POINTS, 1), jnp.float32)
    along_latitude_warmth = jax.random.normal(generator_keys[1], (1, LAYERS, MERIDIAN_POINTS, 1), jnp.float32)
    residual_transport_term = jax.random.normal(generator_keys[2], (SNAPSHOT_TIMES, LAYERS, MERIDIAN_POINTS, 1), jnp.float32)
    thermal_deviate = 0.6 * residual_transport_term + 0.8 * jax.random.normal(generator_keys[3], (SNAPSHOT_TIMES, LAYERS, MERIDIAN_POINTS, 1), jnp.float32)
    steady_share = jax.random.normal(generator_keys[4], (1, LAYERS, MERIDIAN_POINTS, LONGITUDE_SLOTS), jnp.float32)
    steady_warmth = jax.random.normal(generator_keys[5], (1, LAYERS, MERIDIAN_POINTS, LONGITUDE_SLOTS), jnp.float32)
    speed_residual = jax.random.normal(generator_keys[6], (SNAPSHOT_TIMES, LAYERS, MERIDIAN_POINTS, LONGITUDE_SLOTS), jnp.float32)
    thermal_residual = jax.random.normal(generator_keys[7], (SNAPSHOT_TIMES, LAYERS, MERIDIAN_POINTS, LONGITUDE_SLOTS), jnp.float32)
    steady_factor = jax.random.uniform(generator_keys[8], (1, LAYERS, MERIDIAN_POINTS, 1), jnp.float32, -1.0, 1.0)
    fluctuating_factor = jax.random.uniform(generator_keys[9], (1, LAYERS, MERIDIAN_POINTS, 1), jnp.float32, 0.2, 1.0)
    poleward_flow = 0.5 * along_latitude_flow + 0.3 * residual_transport_term + 0.7 * steady_share + speed_residual
    potential_warmth = along_latitude_warmth + 0.3 * thermal_deviate + steady_factor * steady_share + 0.5 * steady_warmth + fluctuating_factor * speed_residual + 0.6 * thermal_residual
    return (jnp.clip(poleward_flow, -16.0, 16.0), jnp.clip(potential_warmth, -16.0, 16.0))


def draw_poleward_flow(key, part):
    return ocean_fields(key)[0]


def draw_potential_warmth(key, part):
    return ocean_fields(key)[1]


def draw_water_profile_flag(key, part):
    columns = jnp.arange(LONGITUDE_SLOTS, dtype=jnp.int32)
    threshold = 25 + 65 * columns // LONGITUDE_SLOTS
    dice = jax.random.randint(jax.random.fold_in(key, 21), (MERIDIAN_POINTS, LONGITUDE_SLOTS), 0, 100)
    return (dice < threshold[None, :]).astype(jnp.int32)


def draw_floor_count(key, part):
    wet_levels = jax.random.randint(jax.random.fold_in(key, 31), (MERIDIAN_POINTS, LONGITUDE_SLOTS), 1, LAYERS + 1)
    land_rows = jax.random.randint(jax.random.fold_in(key, 32), (MERIDIAN_POINTS, 1), 0, 16) == 0
    return jnp.where(land_rows, 0, wet_levels).astype(jnp.int32)


def touch_ends(entries, own_key, low, top_value):
    dims = entries.shape
    index_at = [jax.random.randint(jax.random.fold_in(own_key, axis), (), 0, dims[axis]) for axis in range(len(dims))]
    entries = entries.at[tuple(index_at)].set(low)
    longest = dims.index(max(dims))
    index_at[longest] = (index_at[longest] + 1) % dims[longest]
    return entries.at[tuple(index_at)].set(top_value)


def setup_inputs(seed: int = 0) -> dict:
    key_of = jax.random.split(jax.random.key(seed), 6)
    return {
        "poleward_flow": draw_poleward_flow(jax.random.fold_in(key_of[5], 71), 0),
        "potential_warmth": draw_potential_warmth(jax.random.fold_in(key_of[5], 71), 0),
        "water_profile_flag": draw_water_profile_flag(jax.random.fold_in(key_of[5], 71), 0),
        "floor_count": draw_floor_count(jax.random.fold_in(key_of[5], 71), 0),
        "catchment_label_for_site": touch_ends(jax.random.randint(key_of[4], (MERIDIAN_POINTS, LONGITUDE_SLOTS), 0, BASINS), jax.random.fold_in(key_of[4], 1), 0, BASINS - 1).astype(jnp.int32),
    }


highest_accuracy = lax.Precision.HIGHEST

def layer_summands(layer_position, meridional_speed_layer, thermal_layer_slice, bottom_layer_limit, catchment_label_for_site):
    topmost_warmth = jnp.concatenate([thermal_layer_slice[:, 1:, :], jnp.zeros_like(thermal_layer_slice[:, :1, :])], axis=1)
    warmth_entry = 0.5 * (thermal_layer_slice + topmost_warmth)
    upper_depth = jnp.concatenate([bottom_layer_limit[1:], jnp.zeros_like(bottom_layer_limit[:1])], axis=0)
    level_value = layer_position.astype(jnp.float32)
    wet_cells = ((level_value < bottom_layer_limit) & (level_value < upper_depth)).astype(jnp.float32)
    basin_ids = jnp.arange(BASINS, dtype=jnp.int32)
    one_hot = (catchment_label_for_site[None] == basin_ids[:, None, None]).astype(jnp.float32)
    scaling_factors = one_hot * wet_cells[None]
    watered_total = lax.optimization_barrier(jnp.sum(scaling_factors, axis=2))
    along_latitude_flow = jnp.einsum('qfd,zfd->zqf', scaling_factors, meridional_speed_layer, precision=highest_accuracy)
    along_latitude_warmth = jnp.einsum('qfd,zfd->zqf', scaling_factors, warmth_entry, precision=highest_accuracy)
    means_v = along_latitude_flow / jnp.maximum(watered_total, 1.0)
    averages_heat = along_latitude_warmth / jnp.maximum(watered_total, 1.0)
    bar_v = lax.optimization_barrier(jnp.mean(means_v, axis=0))
    bar_t = lax.optimization_barrier(jnp.mean(averages_heat, axis=0))
    mean_velocity = lax.optimization_barrier(jnp.mean(meridional_speed_layer, axis=0))
    average_warmth = lax.optimization_barrier(jnp.mean(warmth_entry, axis=0))
    bar_v_cells = jnp.einsum('bji,bj->ji', one_hot, bar_v, precision=highest_accuracy)
    averaged_heat_grid = jnp.einsum('bji,bj->ji', one_hot, bar_t, precision=highest_accuracy)
    means_v_cells = jnp.einsum('bji,tbj->tji', one_hot, means_v, precision=highest_accuracy)
    averages_heat_grid = jnp.einsum('bji,tbj->tji', one_hot, averages_heat, precision=highest_accuracy)
    velocity_star = mean_velocity - bar_v_cells
    temp_star = average_warmth - averaged_heat_grid
    velocity_eddy = meridional_speed_layer - mean_velocity - (means_v_cells - bar_v_cells)
    warmth_fluctuation = warmth_entry - average_warmth - (averages_heat_grid - averaged_heat_grid)
    scaling = 1.0 / math.sqrt(LONGITUDE_SLOTS)
    mean_flow = scaling * watered_total * bar_v * bar_t
    steady_share = scaling * jnp.einsum('bji,ji->bj', scaling_factors, velocity_star * temp_star, precision=highest_accuracy)
    zonal_swing = scaling * watered_total * lax.optimization_barrier(jnp.mean((means_v - bar_v) * (averages_heat - bar_t), axis=0))
    transient = scaling * jnp.einsum('bji,ji->bj', scaling_factors, lax.optimization_barrier(jnp.mean(velocity_eddy * warmth_fluctuation, axis=0)), precision=highest_accuracy)
    return (wet_cells * temp_star, jnp.stack([mean_flow, steady_share, zonal_swing, transient]))

def reference(poleward_flow, potential_warmth, water_profile_flag, floor_count, catchment_label_for_site):
    bottom_layer_limit = (water_profile_flag * floor_count).astype(jnp.float32)

    def per_level(layer_position):
        meridional_speed_layer = lax.dynamic_index_in_dim(poleward_flow, layer_position, 1, keepdims=False)
        thermal_layer_slice = lax.dynamic_index_in_dim(potential_warmth, layer_position, 1, keepdims=False)
        return layer_summands(layer_position, meridional_speed_layer, thermal_layer_slice, bottom_layer_limit, catchment_label_for_site)
    eddy_temp, stacked = lax.map(per_level, jnp.arange(LAYERS, dtype=jnp.int32))
    return (eddy_temp, jnp.transpose(stacked, (1, 2, 0, 3)))
```

```python
import functools
import math

import jax
import jax.numpy as jnp
from jax import lax
from jax.experimental import pallas as pl
from jax.experimental.pallas import tpu as pltpu
from jax.sharding import PartitionSpec as P

BASINS = 10
MESH = pl.DeviceIdType.MESH
SUB = 8
LANES = 128


def kernel(
    lat_devices, lon_devices, snapshots, levels, share_rows,
    flow_hbm, warmth_hbm, flag_ref, floor_ref, label_ref,
    eddy_ref, transport_ref,
    flow, warmth, halo_flag, halo_floor, average, dots, stats, received, bars,
    load_flow, load_warmth, halo_send, halo_recv, stat_send, stat_recv, bar_send, bar_recv,
):
    rows = flow.shape[1]
    blocks = rows // SUB
    owners = SUB // share_rows
    planes = snapshots * levels
    lat = lax.axis_index("lat")
    me = lax.axis_index("lon")
    own_block = me // owners
    scaling = 1.0 / math.sqrt(LANES * lon_devices)

    def flow_copy(b):
        at = pl.ds(b * SUB, SUB)
        return pltpu.make_async_copy(flow_hbm.at[:, at, :], flow.at[:, at, :], load_flow.at[b])

    def warmth_copy(b):
        at = pl.ds(b * SUB, SUB)
        return pltpu.make_async_copy(warmth_hbm.at[:, at, :], warmth.at[:, at, :], load_warmth.at[b])

    for b in range(blocks):
        warmth_copy(b).start()
        flow_copy(b).start()

    barrier = pltpu.get_barrier_semaphore()
    for d in range(1, lon_devices):
        pl.semaphore_signal(
            barrier, inc=1, device_id=(lat, lax.rem(me + d, lon_devices)), device_id_type=MESH
        )

    @pl.when(lat > 0)
    def _():
        pl.semaphore_signal(barrier, inc=1, device_id=(lat - 1, me), device_id_type=MESH)

    @pl.when(lat < lat_devices - 1)
    def _():
        pl.semaphore_signal(barrier, inc=1, device_id=(lat + 1, me), device_id_type=MESH)

    greeted = lon_devices - 1 + (lat > 0).astype(jnp.int32) + (lat < lat_devices - 1).astype(jnp.int32)
    pl.semaphore_wait(barrier, greeted)

    halo_to = (jnp.maximum(lat - 1, 0), me)

    def halo_copies():
        pairs = (
            (warmth.at[:, pl.ds(0, 1), :], warmth.at[:, pl.ds(rows, 1), :]),
            (flag_ref.at[pl.ds(0, SUB), :], halo_flag),
            (floor_ref.at[pl.ds(0, SUB), :], halo_floor),
        )
        return [
            pltpu.make_async_remote_copy(
                src_ref=src, dst_ref=dst, send_sem=halo_send.at[n], recv_sem=halo_recv.at[n],
                device_id=halo_to, device_id_type=MESH,
            )
            for n, (src, dst) in enumerate(pairs)
        ]

    for b in range(blocks):
        warmth_copy(b).wait()
        if b == 0:
            @pl.when(lat > 0)
            def _():
                for copy in halo_copies():
                    copy.start()
        flow_copy(b).wait()

    @pl.when(lat < lat_devices - 1)
    def _():
        for copy in halo_copies():
            copy.wait_recv()

    @pl.when(lat == lat_devices - 1)
    def _():
        warmth[:, pl.ds(rows, 1), :] = jnp.zeros((planes, 1, LANES), jnp.float32)
        halo_flag[...] = jnp.zeros_like(halo_flag)
        halo_floor[...] = jnp.zeros_like(halo_floor)

    sub = lax.broadcasted_iota(jnp.int32, (SUB, LANES), 0)
    level = lax.broadcasted_iota(jnp.int32, (levels, SUB, LANES), 0)
    lane_row = lax.rem(lax.broadcasted_iota(jnp.int32, (SUB, LANES), 1), SUB)

    def next_row(here, after):
        first = lax.broadcasted_iota(jnp.int32, here.shape, here.ndim - 2) == 0
        return pltpu.roll(jnp.where(first, after, here), SUB - 1, here.ndim - 2)

    def wet_cells(b):
        at = pl.ds(pl.multiple_of(b * SUB, SUB), SUB)
        after = pl.ds(pl.multiple_of(lax.min(b + 1, blocks - 1) * SUB, SUB), SUB)
        depth = flag_ref[at, :] * floor_ref[at, :]
        inner = flag_ref[after, :] * floor_ref[after, :]
        outer = halo_flag[...] * halo_floor[...]
        limit = jnp.minimum(depth, next_row(depth, jnp.where(b == blocks - 1, outer, inner)))
        return (level < limit[None]).astype(jnp.float32)

    def stat_copy(b, g):
        return pltpu.make_async_remote_copy(
            src_ref=stats.at[b], dst_ref=received.at[me],
            send_sem=stat_send.at[b, g], recv_sem=stat_recv.at[me],
            device_id=(lat, b * owners + g), device_id_type=MESH,
        )

    def block_stats(s, carry):
        b = lax.rem(own_block + 1 + s, blocks)
        at = pl.ds(pl.multiple_of(b * SUB, SUB), SUB)
        after = pl.ds(pl.multiple_of(b * SUB + SUB, SUB), SUB)
        wet = wet_cells(b)
        velocity = flow[:, at, :].reshape(snapshots, levels, SUB, LANES)
        here = warmth[:, at, :]
        point = (0.5 * (here + next_row(here, warmth[:, after, :]))).reshape(
            snapshots, levels, SUB, LANES
        )
        mean_velocity = jnp.sum(velocity, axis=0) * (1.0 / snapshots)
        mean_warmth = jnp.sum(point, axis=0) * (1.0 / snapshots)
        cross = jnp.sum((velocity - mean_velocity) * (point - mean_warmth), axis=0) * (1.0 / snapshots)
        average[:, at, :] = mean_warmth
        fields = jnp.concatenate(
            [
                (velocity * wet[None]).reshape(planes, SUB, LANES),
                (point * wet[None]).reshape(planes, SUB, LANES),
                wet,
                wet,
                mean_velocity * mean_warmth * wet,
                cross * wet,
            ],
            axis=0,
        ).reshape(-1, LANES)
        high = fields.astype(jnp.bfloat16)
        low = (fields - high.astype(jnp.float32)).astype(jnp.bfloat16)
        labels = label_ref[at, :]
        member = jnp.concatenate(
            [(labels == n).astype(jnp.float32) for n in range(LANES // SUB)], axis=0
        ).astype(jnp.bfloat16)
        dots[...] = lax.dot_general(
            jnp.concatenate([high, low], axis=1), jnp.concatenate([member, member], axis=1),
            (((1,), (1,)), ((), ())), preferred_element_type=jnp.float32,
        )
        count = stats.shape[1]
        lanes = lax.rem(lax.broadcasted_iota(jnp.int32, (count, LANES), 1), SUB)
        gathered = dots[pl.ds(0, count, stride=SUB), :]
        for j in range(1, SUB):
            gathered = jnp.where(lanes == j, dots[pl.ds(j, count, stride=SUB), :], gathered)
        stats[pl.ds(b, 1)] = gathered[None]
        for g in range(owners):
            @pl.when(b * owners + g != me)
            def _():
                stat_copy(b, g).start()
        return carry

    lax.fori_loop(0, blocks, block_stats, 0)

    def add_received(d, total):
        src = lax.rem(me + lon_devices - d, lon_devices)
        pltpu.make_async_remote_copy(
            src_ref=stats.at[0], dst_ref=received.at[src],
            send_sem=stat_send.at[0, 0], recv_sem=stat_recv.at[src],
            device_id=(lat, src), device_id_type=MESH,
        ).wait_recv()
        return total + received[pl.ds(src, 1)][0]

    total = lax.fori_loop(1, lon_devices, add_received, stats[pl.ds(own_block, 1)][0])

    def both_halves(x):
        return x + pltpu.roll(x, levels, 0)

    count = total[2 * planes : 2 * planes + SUB]
    divisor = jnp.maximum(count, 1.0)
    means_v = total[:planes].reshape(planes // SUB, SUB, LANES) / divisor
    means_t = total[planes : 2 * planes].reshape(planes // SUB, SUB, LANES) / divisor
    bar_v = both_halves(jnp.sum(means_v, axis=0)) * (1.0 / snapshots)
    bar_t = both_halves(jnp.sum(means_t, axis=0)) * (1.0 / snapshots)

    def bar_copy(block, device, n):
        return pltpu.make_async_remote_copy(
            src_ref=bars.at[block], dst_ref=bars.at[block],
            send_sem=bar_send.at[n], recv_sem=bar_recv.at[block],
            device_id=(lat, device), device_id_type=MESH,
        )

    leads = lax.rem(me, owners) == 0

    @pl.when(leads)
    def _():
        bars[pl.ds(own_block, 1)] = bar_t[None]
        for d in range(1, lon_devices):
            bar_copy(own_block, lax.rem(me + d, lon_devices), d).start()

    swing = both_halves(jnp.sum((means_v - bar_v) * (means_t - bar_t), axis=0)) * (1.0 / snapshots)
    upper = jnp.where(sub < levels, scaling * count * bar_v * bar_t, scaling * count * swing)
    lower = scaling * total[2 * planes + SUB : 2 * planes + 2 * SUB] - upper
    if owners > 1:
        shift = LANES - lax.rem(me, owners) * share_rows
        upper = pltpu.roll(upper, shift, 1)
        lower = pltpu.roll(lower, shift, 1)
    for n in range(BASINS):
        lanes = slice(n * SUB, n * SUB + share_rows)
        transport_ref[0, n] = upper[:levels, lanes]
        transport_ref[1, n] = lower[:levels, lanes]
        transport_ref[2, n] = upper[levels:, lanes]
        transport_ref[3, n] = lower[levels:, lanes]

    for b in range(blocks):
        @pl.when(jnp.logical_or(own_block != b, jnp.logical_not(leads)))
        def _():
            bar_copy(b, b * owners, 0).wait_recv()
        at = pl.ds(b * SUB, SUB)
        wet = wet_cells(b)
        index = label_ref[at, :] * SUB + sub
        bar = bars[b]
        for k in range(levels):
            cells = jnp.take_along_axis(
                jnp.broadcast_to(bar[k : k + 1], (SUB, LANES)), index, axis=1
            )
            eddy_ref[k, at, :] = wet[k] * (average[k, at, :] - cells)

    @pl.when(lat > 0)
    def _():
        for copy in halo_copies():
            copy.wait_send()

    for b in range(blocks):
        for g in range(owners):
            @pl.when(b * owners + g != me)
            def _():
                stat_copy(b, g).wait_send()

    @pl.when(leads)
    def _():
        for d in range(1, lon_devices):
            bar_copy(own_block, lax.rem(me + d, lon_devices), d).wait_send()


def shards(
    lat_devices, lon_devices,
    poleward_flow, potential_warmth, water_profile_flag, floor_count, catchment_label_for_site,
):
    snapshots, levels, rows, columns = poleward_flow.shape
    share_rows = rows // lon_devices
    blocks = rows // SUB
    planes = snapshots * levels
    owners = SUB // share_rows
    fields = 2 * planes + 4 * levels
    f32, vmem, dma = jnp.float32, pltpu.VMEM, pltpu.SemaphoreType.DMA
    return pl.pallas_call(
        functools.partial(kernel, lat_devices, lon_devices, snapshots, levels, share_rows),
        out_shape=(
            jax.ShapeDtypeStruct((levels, rows, columns), f32),
            jax.ShapeDtypeStruct((4, BASINS, levels, share_rows), f32),
        ),
        in_specs=[pl.BlockSpec(memory_space=pl.ANY)] * 2 + [pl.BlockSpec(memory_space=vmem)] * 3,
        out_specs=(pl.BlockSpec(memory_space=vmem), pl.BlockSpec(memory_space=vmem)),
        scratch_shapes=[
            vmem((planes, rows, columns), f32),
            vmem((planes, rows + SUB, columns), f32),
            vmem((SUB, columns), jnp.int32),
            vmem((SUB, columns), jnp.int32),
            vmem((levels, rows, columns), f32),
            vmem((fields * SUB, LANES), f32),
            vmem((blocks, fields, LANES), f32),
            vmem((lon_devices, fields, LANES), f32),
            vmem((blocks, SUB, LANES), f32),
            dma((blocks,)),
            dma((blocks,)),
            dma((3,)),
            dma((3,)),
            dma((blocks, owners)),
            dma((lon_devices,)),
            dma((lon_devices,)),
            dma((blocks,)),
        ],
        compiler_params=pltpu.CompilerParams(collective_id=0, has_side_effects=True),
        name="heat_transport",
    )(
        poleward_flow.reshape(planes, rows, columns),
        potential_warmth.reshape(planes, rows, columns),
        water_profile_flag,
        floor_count,
        catchment_label_for_site,
    )


def solution(mesh):
    return jax.shard_map(
        functools.partial(shards, mesh.shape["lat"], mesh.shape["lon"]),
        mesh=mesh,
        in_specs=(
            P(None, None, "lat", "lon"),
            P(None, None, "lat", "lon"),
            P("lat", "lon"),
            P("lat", "lon"),
            P("lat", "lon"),
        ),
        out_specs=(P(None, "lat", "lon"), P(None, None, None, ("lat", "lon"))),
        check_vma=False,
    )
```

```python
import functools
import math

import jax
import jax.numpy as jnp
from jax import lax
from jax.experimental import pallas as pl
from jax.experimental.pallas import tpu as pltpu
from jax.sharding import PartitionSpec as P

BASINS = 10
MESH = pl.DeviceIdType.MESH
SUB = 8
LANES = 128


def kernel(
    lat_devices, lon_devices, snapshots, levels, share_rows,
    flow_hbm, warmth_hbm, flag_hbm, floor_hbm, label_hbm,
    eddy_ref, transport_ref,
    flag_ref, floor_ref, label_ref,
    flow, warmth, average, dots, stats, received, bars,
    load_flow, load_warmth, load_columns, halo_send, halo_recv, stat_send, stat_recv, bar_send, bar_recv,
):
    rows = flow.shape[1]
    blocks = rows // SUB
    owners = SUB // share_rows
    planes = snapshots * levels
    lat = lax.axis_index("lat")
    me = lax.axis_index("lon")
    own_block = me // owners
    scaling = 1.0 / math.sqrt(LANES * lon_devices)

    def block_at(s):
        late = own_block + 2 == blocks
        s = jnp.where(jnp.logical_and(late, s < 2), 1 - s, s)
        return lax.rem(own_block + 1 + s, blocks)

    def flow_copy(b):
        at = pl.ds(pl.multiple_of(b * SUB, SUB), SUB)
        return pltpu.make_async_copy(flow_hbm.at[:, at, :], flow.at[:, at, :], load_flow.at[b])

    def warmth_copy(b):
        at = pl.ds(b * SUB, SUB)
        return pltpu.make_async_copy(warmth_hbm.at[:, at, :], warmth.at[:, at, :], load_warmth.at[b])

    columns = [
        pltpu.make_async_copy(src, dst, load_columns.at[n])
        for n, (src, dst) in enumerate(
            ((flag_hbm, flag_ref.at[pl.ds(0, rows), :]), (floor_hbm, floor_ref.at[pl.ds(0, rows), :]), (label_hbm, label_ref))
        )
    ]
    for copy in columns:
        copy.start()
    for b in range(blocks):
        warmth_copy(b).start()
    for s in range(blocks):
        flow_copy(block_at(s)).start()

    barrier = pltpu.get_barrier_semaphore()
    for d in range(1, lon_devices):
        pl.semaphore_signal(
            barrier, inc=1, device_id=(lat, lax.rem(me + d, lon_devices)), device_id_type=MESH
        )

    @pl.when(lat > 0)
    def _():
        pl.semaphore_signal(barrier, inc=1, device_id=(lat - 1, me), device_id_type=MESH)

    @pl.when(lat < lat_devices - 1)
    def _():
        pl.semaphore_signal(barrier, inc=1, device_id=(lat + 1, me), device_id_type=MESH)

    greeted = lon_devices - 1 + (lat > 0).astype(jnp.int32) + (lat < lat_devices - 1).astype(jnp.int32)
    pl.semaphore_wait(barrier, greeted)

    halo_to = (jnp.maximum(lat - 1, 0), me)

    def halo_copies():
        pairs = (
            (warmth.at[:, pl.ds(0, 1), :], warmth.at[:, pl.ds(rows, 1), :]),
            (flag_ref.at[pl.ds(0, SUB), :], flag_ref.at[pl.ds(rows, SUB), :]),
            (floor_ref.at[pl.ds(0, SUB), :], floor_ref.at[pl.ds(rows, SUB), :]),
        )
        return [
            pltpu.make_async_remote_copy(
                src_ref=src, dst_ref=dst, send_sem=halo_send.at[n], recv_sem=halo_recv.at[n],
                device_id=halo_to, device_id_type=MESH,
            )
            for n, (src, dst) in enumerate(pairs)
        ]

    for copy in columns:
        copy.wait()
    for b in range(blocks):
        warmth_copy(b).wait()

    @pl.when(lat > 0)
    def _():
        for copy in halo_copies():
            copy.start()

    @pl.when(lat == lat_devices - 1)
    def _():
        warmth[:, pl.ds(rows, 1), :] = jnp.zeros((planes, 1, LANES), jnp.float32)
        flag_ref[pl.ds(rows, SUB), :] = jnp.zeros((SUB, LANES), jnp.int32)
        floor_ref[pl.ds(rows, SUB), :] = jnp.zeros((SUB, LANES), jnp.int32)

    sub = lax.broadcasted_iota(jnp.int32, (SUB, LANES), 0)
    level = lax.broadcasted_iota(jnp.int32, (levels, SUB, LANES), 0)
    lane_row = lax.rem(lax.broadcasted_iota(jnp.int32, (SUB, LANES), 1), SUB)

    def next_row(here, after):
        first = lax.broadcasted_iota(jnp.int32, here.shape, here.ndim - 2) == 0
        return pltpu.roll(jnp.where(first, after, here), SUB - 1, here.ndim - 2)

    def wet_cells(b):
        at = pl.ds(pl.multiple_of(b * SUB, SUB), SUB)
        after = pl.ds(pl.multiple_of(b * SUB + SUB, SUB), SUB)
        depth = flag_ref[at, :] * floor_ref[at, :]
        inner = flag_ref[after, :] * floor_ref[after, :]
        limit = jnp.minimum(depth, next_row(depth, inner))
        return (level < limit[None]).astype(jnp.float32)

    def stat_copy(b, g):
        return pltpu.make_async_remote_copy(
            src_ref=stats.at[b], dst_ref=received.at[me],
            send_sem=stat_send.at[b, g], recv_sem=stat_recv.at[me],
            device_id=(lat, b * owners + g), device_id_type=MESH,
        )

    def block_stats(s, carry):
        b = block_at(s)

        @pl.when(jnp.logical_and(b == blocks - 1, lat < lat_devices - 1))
        def _():
            for copy in halo_copies():
                copy.wait_recv()

        flow_copy(b).wait()
        at = pl.ds(pl.multiple_of(b * SUB, SUB), SUB)
        after = pl.ds(pl.multiple_of(b * SUB + SUB, SUB), SUB)
        wet = wet_cells(b)
        velocity = flow[:, at, :].reshape(snapshots, levels, SUB, LANES)
        here = warmth[:, at, :]
        point = (0.5 * (here + next_row(here, warmth[:, after, :]))).reshape(
            snapshots, levels, SUB, LANES
        )
        mean_velocity = jnp.sum(velocity, axis=0) * (1.0 / snapshots)
        mean_warmth = jnp.sum(point, axis=0) * (1.0 / snapshots)
        cross = jnp.sum((velocity - mean_velocity) * (point - mean_warmth), axis=0) * (1.0 / snapshots)
        average[:, at, :] = mean_warmth
        fields = jnp.concatenate(
            [
                (velocity * wet[None]).reshape(planes, SUB, LANES),
                (point * wet[None]).reshape(planes, SUB, LANES),
                wet,
                wet,
                mean_velocity * mean_warmth * wet,
                cross * wet,
            ],
            axis=0,
        ).reshape(-1, LANES)
        high = fields.astype(jnp.bfloat16)
        low = (fields - high.astype(jnp.float32)).astype(jnp.bfloat16)
        labels = label_ref[at, :]
        member = jnp.concatenate(
            [(labels == n).astype(jnp.float32) for n in range(LANES // SUB)], axis=0
        ).astype(jnp.bfloat16)
        dots[...] = lax.dot_general(
            jnp.concatenate([high, low], axis=1), jnp.concatenate([member, member], axis=1),
            (((1,), (1,)), ((), ())), preferred_element_type=jnp.float32,
        )
        count = stats.shape[1]
        lanes = lax.rem(lax.broadcasted_iota(jnp.int32, (count, LANES), 1), SUB)
        gathered = dots[pl.ds(0, count, stride=SUB), :]
        for j in range(1, SUB):
            gathered = jnp.where(lanes == j, dots[pl.ds(j, count, stride=SUB), :], gathered)
        stats[pl.ds(b, 1)] = gathered[None]
        for g in range(owners):
            @pl.when(b * owners + g != me)
            def _():
                stat_copy(b, g).start()
        return carry

    lax.fori_loop(0, blocks, block_stats, 0)

    def add_received(d, total):
        src = lax.rem(me + lon_devices - d, lon_devices)
        pltpu.make_async_remote_copy(
            src_ref=stats.at[0], dst_ref=received.at[src],
            send_sem=stat_send.at[0, 0], recv_sem=stat_recv.at[src],
            device_id=(lat, src), device_id_type=MESH,
        ).wait_recv()
        return total + received[pl.ds(src, 1)][0]

    total = lax.fori_loop(1, lon_devices, add_received, stats[pl.ds(own_block, 1)][0])

    def both_halves(x):
        return x + pltpu.roll(x, levels, 0)

    count = total[2 * planes : 2 * planes + SUB]
    divisor = jnp.maximum(count, 1.0)
    means_v = total[:planes].reshape(planes // SUB, SUB, LANES) / divisor
    means_t = total[planes : 2 * planes].reshape(planes // SUB, SUB, LANES) / divisor
    bar_v = both_halves(jnp.sum(means_v, axis=0)) * (1.0 / snapshots)
    bar_t = both_halves(jnp.sum(means_t, axis=0)) * (1.0 / snapshots)

    def bar_copy(block, device, n):
        return pltpu.make_async_remote_copy(
            src_ref=bars.at[block], dst_ref=bars.at[block],
            send_sem=bar_send.at[n], recv_sem=bar_recv.at[block],
            device_id=(lat, device), device_id_type=MESH,
        )

    leads = lax.rem(me, owners) == 0

    @pl.when(leads)
    def _():
        bars[pl.ds(own_block, 1)] = bar_t[None]
        for d in range(1, lon_devices):
            bar_copy(own_block, lax.rem(me + d, lon_devices), d).start()

    swing = both_halves(jnp.sum((means_v - bar_v) * (means_t - bar_t), axis=0)) * (1.0 / snapshots)
    upper = jnp.where(sub < levels, scaling * count * bar_v * bar_t, scaling * count * swing)
    lower = scaling * total[2 * planes + SUB : 2 * planes + 2 * SUB] - upper
    if owners > 1:
        shift = LANES - lax.rem(me, owners) * share_rows
        upper = pltpu.roll(upper, shift, 1)
        lower = pltpu.roll(lower, shift, 1)
    spread = lax.rem(lax.broadcasted_iota(jnp.int32, (SUB, LANES), 1) * SUB + sub, LANES)
    for c, part in enumerate((upper, lower, upper, lower)):
        for k in range(levels):
            row = c // 2 * levels + k
            table = jnp.take_along_axis(
                jnp.broadcast_to(part[row : row + 1], (SUB, LANES)), spread, axis=1
            )
            transport_ref[c, k] = table[:share_rows, :BASINS]

    for b in range(blocks):
        @pl.when(jnp.logical_or(own_block != b, jnp.logical_not(leads)))
        def _():
            bar_copy(b, b * owners, 0).wait_recv()
        at = pl.ds(b * SUB, SUB)
        wet = wet_cells(b)
        index = label_ref[at, :] * SUB + sub
        bar = bars[b]
        for k in range(levels):
            cells = jnp.take_along_axis(
                jnp.broadcast_to(bar[k : k + 1], (SUB, LANES)), index, axis=1
            )
            eddy_ref[k, at, :] = wet[k] * (average[k, at, :] - cells)

    @pl.when(lat > 0)
    def _():
        for copy in halo_copies():
            copy.wait_send()

    for b in range(blocks):
        for g in range(owners):
            @pl.when(b * owners + g != me)
            def _():
                stat_copy(b, g).wait_send()

    @pl.when(leads)
    def _():
        for d in range(1, lon_devices):
            bar_copy(own_block, lax.rem(me + d, lon_devices), d).wait_send()


def shards(
    lat_devices, lon_devices,
    poleward_flow, potential_warmth, water_profile_flag, floor_count, catchment_label_for_site,
):
    snapshots, levels, rows, columns = poleward_flow.shape
    share_rows = rows // lon_devices
    blocks = rows // SUB
    planes = snapshots * levels
    owners = SUB // share_rows
    fields = 2 * planes + 4 * levels
    f32, vmem, dma = jnp.float32, pltpu.VMEM, pltpu.SemaphoreType.DMA
    eddy_temp, transport = pl.pallas_call(
        functools.partial(kernel, lat_devices, lon_devices, snapshots, levels, share_rows),
        out_shape=(
            vmem((levels, rows, columns), f32),
            vmem((4, levels, share_rows, BASINS), f32),
        ),
        in_specs=[pl.BlockSpec(memory_space=pltpu.HBM)] * 5,
        out_specs=(pl.BlockSpec(memory_space=vmem), pl.BlockSpec(memory_space=vmem)),
        scratch_shapes=[
            vmem((rows + SUB, columns), jnp.int32),
            vmem((rows + SUB, columns), jnp.int32),
            vmem((rows, columns), jnp.int32),
            vmem((planes, rows, columns), f32),
            vmem((planes, rows + SUB, columns), f32),
            vmem((levels, rows, columns), f32),
            vmem((fields * SUB, LANES), f32),
            vmem((blocks, fields, LANES), f32),
            vmem((lon_devices, fields, LANES), f32),
            vmem((blocks, SUB, LANES), f32),
            dma((blocks,)),
            dma((blocks,)),
            dma((3,)),
            dma((3,)),
            dma((3,)),
            dma((blocks, owners)),
            dma((lon_devices,)),
            dma((lon_devices,)),
            dma((blocks,)),
        ],
        compiler_params=pltpu.CompilerParams(collective_id=0, has_side_effects=True, vmem_limit_bytes=62 * 1024 * 1024),
        name="heat_transport",
    )(
        poleward_flow.reshape(planes, rows, columns),
        potential_warmth.reshape(planes, rows, columns),
        water_profile_flag,
        floor_count,
        catchment_label_for_site,
    )
    return eddy_temp, jnp.transpose(transport, (0, 3, 1, 2))


def solution(mesh):
    return jax.shard_map(
        functools.partial(shards, mesh.shape["lat"], mesh.shape["lon"]),
        mesh=mesh,
        in_specs=(
            P(None, None, "lat", "lon"),
            P(None, None, "lat", "lon"),
            P("lat", "lon"),
            P("lat", "lon"),
            P("lat", "lon"),
        ),
        out_specs=(P(None, "lat", "lon"), P(None, None, None, ("lat", "lon"))),
        check_vma=False,
    )
```

```python
import functools
import math

import jax
import jax.numpy as jnp
from jax import lax
from jax.experimental import pallas as pl
from jax.experimental.pallas import tpu as pltpu
from jax.sharding import PartitionSpec as P

BASINS = 10
MESH = pl.DeviceIdType.MESH
SUB = 8
LANES = 128


def kernel(
    lat_devices, lon_devices, snapshots, levels, share_rows,
    flow_hbm, warmth_hbm, flag_hbm, floor_hbm, label_hbm,
    eddy_ref, transport_ref,
    flag_ref, floor_ref, label_ref, depth, flow, warmth, average, dots,
    halo_out, halo_in, stats, received, sums, peer_sums,
    load_flow, load_warmth, load_columns, halo_send, halo_recv,
    stat_send, stat_recv, sum_send, sum_recv,
):
    rows = flow.shape[1]
    blocks = rows // SUB
    last = blocks - 1
    owners = SUB // share_rows
    planes = snapshots * levels
    packed = stats.shape[1]
    fields = dots.shape[0] // SUB
    used = BASINS * SUB
    lat = lax.axis_index("lat")
    me = lax.axis_index("lon")
    own_block = me // owners
    scaling = 1.0 / math.sqrt(LANES * lon_devices)

    def window(b):
        return pl.ds(pl.multiple_of(b * SUB, SUB), SUB)

    def flow_copy(b):
        at = window(b)
        return pltpu.make_async_copy(flow_hbm.at[:, at, :], flow.at[:, at, :], load_flow.at[b])

    def warmth_copy(b):
        at = window(b)
        return pltpu.make_async_copy(warmth_hbm.at[:, at, :], warmth.at[:, at, :], load_warmth.at[b])

    columns = [
        pltpu.make_async_copy(src, dst, load_columns.at[n])
        for n, (src, dst) in enumerate(
            ((flag_hbm, flag_ref), (floor_hbm, floor_ref), (label_hbm, label_ref))
        )
    ]
    for copy in columns:
        copy.start()
    for b in range(blocks):
        warmth_copy(b).start()
        flow_copy(b).start()

    barrier = pltpu.get_barrier_semaphore()

    def greet(d, carry):
        pl.semaphore_signal(
            barrier, inc=1, device_id=(lat, lax.rem(me + d, lon_devices)), device_id_type=MESH
        )
        return carry

    @pl.when(lat > 0)
    def _():
        pl.semaphore_signal(barrier, inc=1, device_id=(lat - 1, me), device_id_type=MESH)

    @pl.when(lat < lat_devices - 1)
    def _():
        pl.semaphore_signal(barrier, inc=1, device_id=(lat + 1, me), device_id_type=MESH)

    lax.fori_loop(1, lon_devices, greet, 0)

    halo_copy = pltpu.make_async_remote_copy(
        src_ref=halo_out, dst_ref=halo_in, send_sem=halo_send, recv_sem=halo_recv,
        device_id=(jnp.maximum(lat - 1, 0), me), device_id_type=MESH,
    )

    def sum_copy(to, source, part):
        span = pl.ds(0, last) if part == 0 else pl.ds(last, 1)
        return pltpu.make_async_remote_copy(
            src_ref=sums.at[span], dst_ref=peer_sums.at[source, span],
            send_sem=sum_send.at[part, to], recv_sem=sum_recv.at[part, source],
            device_id=(lat, to), device_id_type=MESH,
        )

    def stat_copy(b, to, source):
        return pltpu.make_async_remote_copy(
            src_ref=stats.at[b], dst_ref=received.at[source],
            send_sem=stat_send.at[to], recv_sem=stat_recv.at[source],
            device_id=(lat, to), device_id_type=MESH,
        )

    def each_peer(action):
        def step(d, carry):
            action(lax.rem(me + d, lon_devices))
            return carry

        lax.fori_loop(1, lon_devices, step, 0)

    sub = lax.broadcasted_iota(jnp.int32, (SUB, LANES), 0)
    level = lax.broadcasted_iota(jnp.int32, (levels, SUB, LANES), 0).astype(jnp.float32)

    def next_row(here, after):
        first = lax.broadcasted_iota(jnp.int32, here.shape, here.ndim - 2) == 0
        return pltpu.roll(jnp.where(first, after, here), SUB - 1, here.ndim - 2)

    def both_halves(x):
        return x + pltpu.roll(x, levels, 0)

    def wet_cells(b):
        here = depth[window(b), :]
        limit = jnp.minimum(here, next_row(here, depth[window(b + 1), :]))
        return (level < limit[None]).astype(jnp.float32)

    def block_stats(b, carry):
        at = window(b)
        wet = wet_cells(b)
        velocity = flow[:, at, :].reshape(snapshots, levels, SUB, LANES)
        here = warmth[:, at, :]
        point = (0.5 * (here + next_row(here, warmth[:, window(b + 1), :]))).reshape(
            snapshots, levels, SUB, LANES
        )
        mean_velocity = jnp.sum(velocity, axis=0) * (1.0 / snapshots)
        mean_warmth = jnp.sum(point, axis=0) * (1.0 / snapshots)
        cross = jnp.sum((velocity - mean_velocity) * (point - mean_warmth), axis=0) * (1.0 / snapshots)
        average[:, at, :] = mean_warmth
        values = jnp.concatenate(
            [
                (velocity * wet[None]).reshape(planes, SUB, LANES),
                (point * wet[None]).reshape(planes, SUB, LANES),
                wet,
                wet,
                mean_velocity * mean_warmth * wet,
                cross * wet,
            ],
            axis=0,
        ).reshape(-1, LANES)
        high = values.astype(jnp.bfloat16)
        low = (values - high.astype(jnp.float32)).astype(jnp.bfloat16)
        labels = label_ref[at, :]
        member = jnp.concatenate(
            [(labels == n).astype(jnp.float32) for n in range(LANES // SUB)], axis=0
        ).astype(jnp.bfloat16)
        dots[...] = lax.dot_general(
            jnp.concatenate([high, low], axis=1), jnp.concatenate([member, member], axis=1),
            (((1,), (1,)), ((), ())), preferred_element_type=jnp.float32,
        )
        row_of = lax.rem(lax.broadcasted_iota(jnp.int32, (fields, LANES), 1), SUB)
        zonal = dots[pl.ds(0, fields, stride=SUB), :]
        for j in range(1, SUB):
            zonal = jnp.where(row_of == j, dots[pl.ds(j, fields, stride=SUB), :], zonal)
        warmth_sum = both_halves(
            jnp.sum(zonal[planes : 2 * planes].reshape(planes // SUB, SUB, LANES), axis=0)
        )
        count = zonal[2 * planes : 2 * planes + SUB]
        sums[pl.ds(b, 1)] = jnp.where(sub < levels, warmth_sum, count)[None]
        half = packed // 2
        rest = zonal[packed:]
        spare = lax.broadcasted_iota(jnp.int32, (half, LANES), 1) >= used
        stats[pl.ds(b, 1)] = jnp.concatenate(
            [
                jnp.where(spare, pltpu.roll(rest, used, 1), zonal[:half]),
                jnp.where(spare, pltpu.roll(rest, 2 * used - LANES, 1), zonal[half:packed]),
            ],
            axis=0,
        )[None]
        return carry

    for copy in columns:
        copy.wait()
    depth[pl.ds(0, rows), :] = (flag_ref[...] * floor_ref[...]).astype(jnp.float32)
    for b in range(blocks):
        warmth_copy(b).wait()
    halo_out[pl.ds(0, planes), :] = warmth[:, 0, :]
    halo_out[pl.ds(planes, SUB), :] = depth[pl.ds(0, SUB), :]

    def early_block(b, carry):
        flow_copy(b).wait()
        return block_stats(b, carry)

    lax.fori_loop(0, last, early_block, 0)

    pl.semaphore_wait(
        barrier,
        lon_devices - 1 + (lat > 0).astype(jnp.int32) + (lat < lat_devices - 1).astype(jnp.int32),
    )

    @pl.when(lat > 0)
    def _():
        halo_copy.start()

    each_peer(lambda to: sum_copy(to, me, 0).start())

    def send_stats(to):
        @pl.when(to // owners < last)
        def _():
            stat_copy(to // owners, to, me).start()

    each_peer(send_stats)
    flow_copy(last).wait()

    @pl.when(lat < lat_devices - 1)
    def _():
        halo_copy.wait_recv()
        warmth[:, rows, :] = halo_in[pl.ds(0, planes), :]
        depth[pl.ds(rows, SUB), :] = halo_in[pl.ds(planes, SUB), :]

    @pl.when(lat == lat_devices - 1)
    def _():
        warmth[:, rows, :] = jnp.zeros((planes, LANES), jnp.float32)
        depth[pl.ds(rows, SUB), :] = jnp.zeros((SUB, LANES), jnp.float32)

    block_stats(last, 0)
    each_peer(lambda to: sum_copy(to, me, 1).start())

    def send_last(to):
        @pl.when(to // owners == last)
        def _():
            stat_copy(last, to, me).start()

    each_peer(send_last)

    def add_sums(d, total):
        source = lax.rem(me + lon_devices - d, lon_devices)
        sum_copy(me, source, 0).wait_recv()
        sum_copy(me, source, 1).wait_recv()
        return total + peer_sums[pl.ds(source, 1)][0]

    all_sums = lax.fori_loop(1, lon_devices, add_sums, sums[...])
    for b in range(blocks):
        at = pl.ds(b * SUB, SUB)
        wet = wet_cells(b)
        index = label_ref[at, :] * SUB + sub
        bar = all_sums[b] / jnp.maximum(pltpu.roll(all_sums[b], levels, 0), 1.0) * (1.0 / snapshots)
        for k in range(levels):
            cells = jnp.take_along_axis(
                jnp.broadcast_to(bar[k : k + 1], (SUB, LANES)), index, axis=1
            )
            eddy_ref[k, at, :] = wet[k] * (average[k, at, :] - cells)

    def add_received(d, total):
        source = lax.rem(me + lon_devices - d, lon_devices)
        stat_copy(0, me, source).wait_recv()
        return total + received[pl.ds(source, 1)][0]

    total = lax.fori_loop(1, lon_devices, add_received, stats[pl.ds(own_block, 1)][0])
    half = packed // 2
    lane = lax.broadcasted_iota(jnp.int32, (half, LANES), 1)
    total = jnp.concatenate(
        [
            total,
            jnp.where(
                lane < LANES - used,
                pltpu.roll(total[:half], LANES - used, 1),
                pltpu.roll(total[half:], 2 * LANES - 2 * used, 1),
            ),
        ],
        axis=0,
    )
    count = total[2 * planes : 2 * planes + SUB]
    divisor = jnp.maximum(count, 1.0)
    means_v = total[:planes].reshape(planes // SUB, SUB, LANES) / divisor
    means_t = total[planes : 2 * planes].reshape(planes // SUB, SUB, LANES) / divisor
    bar_v = both_halves(jnp.sum(means_v, axis=0)) * (1.0 / snapshots)
    bar_t = both_halves(jnp.sum(means_t, axis=0)) * (1.0 / snapshots)
    swing = both_halves(jnp.sum((means_v - bar_v) * (means_t - bar_t), axis=0)) * (1.0 / snapshots)
    upper = jnp.where(sub < levels, scaling * count * bar_v * bar_t, scaling * count * swing)
    lower = scaling * total[2 * planes + SUB : 2 * planes + 2 * SUB] - upper
    if owners > 1:
        shift = LANES - lax.rem(me, owners) * share_rows
        upper = pltpu.roll(upper, shift, 1)
        lower = pltpu.roll(lower, shift, 1)
    spread = lax.rem(lax.broadcasted_iota(jnp.int32, (SUB, LANES), 1) * SUB + sub, LANES)
    for c, part in enumerate((upper, lower, upper, lower)):
        for k in range(levels):
            row = c // 2 * levels + k
            table = jnp.take_along_axis(
                jnp.broadcast_to(part[row : row + 1], (SUB, LANES)), spread, axis=1
            )
            transport_ref[c, k] = table[:share_rows, :BASINS]

    @pl.when(lat > 0)
    def _():
        halo_copy.wait_send()

    def sent(to):
        sum_copy(to, me, 0).wait_send()
        sum_copy(to, me, 1).wait_send()
        stat_copy(to // owners, to, me).wait_send()

    each_peer(sent)


def shards(
    lat_devices, lon_devices,
    poleward_flow, potential_warmth, water_profile_flag, floor_count, catchment_label_for_site,
):
    snapshots, levels, rows, columns = poleward_flow.shape
    share_rows = rows // lon_devices
    blocks = rows // SUB
    planes = snapshots * levels
    fields = 2 * planes + 4 * levels
    packed = fields * 2 // 3
    f32, i32, vmem, dma = jnp.float32, jnp.int32, pltpu.VMEM, pltpu.SemaphoreType.DMA
    eddy_temp, transport = pl.pallas_call(
        functools.partial(kernel, lat_devices, lon_devices, snapshots, levels, share_rows),
        out_shape=(
            vmem((levels, rows, columns), f32),
            vmem((4, levels, share_rows, BASINS), f32),
        ),
        in_specs=[pl.BlockSpec(memory_space=pltpu.HBM)] * 5,
        out_specs=(pl.BlockSpec(memory_space=vmem), pl.BlockSpec(memory_space=vmem)),
        scratch_shapes=[
            vmem((rows, columns), i32),
            vmem((rows, columns), i32),
            vmem((rows, columns), i32),
            vmem((rows + SUB, columns), f32),
            vmem((planes, rows, columns), f32),
            vmem((planes, rows + SUB, columns), f32),
            vmem((levels, rows, columns), f32),
            vmem((fields * SUB, LANES), f32),
            vmem((planes + SUB, LANES), f32),
            vmem((planes + SUB, LANES), f32),
            vmem((blocks, packed, LANES), f32),
            vmem((lon_devices, packed, LANES), f32),
            vmem((blocks, SUB, LANES), f32),
            vmem((lon_devices, blocks, SUB, LANES), f32),
            dma((blocks,)),
            dma((blocks,)),
            dma((3,)),
            dma,
            dma,
            dma((lon_devices,)),
            dma((lon_devices,)),
            dma((2, lon_devices)),
            dma((2, lon_devices)),
        ],
        compiler_params=pltpu.CompilerParams(
            collective_id=0, has_side_effects=True, vmem_limit_bytes=62 * 1024 * 1024
        ),
        name="heat_transport",
    )(
        poleward_flow.reshape(planes, rows, columns),
        potential_warmth.reshape(planes, rows, columns),
        water_profile_flag,
        floor_count,
        catchment_label_for_site,
    )
    return eddy_temp, jnp.transpose(transport, (0, 3, 1, 2))


def solution(mesh):
    return jax.shard_map(
        functools.partial(shards, mesh.shape["lat"], mesh.shape["lon"]),
        mesh=mesh,
        in_specs=(
            P(None, None, "lat", "lon"),
            P(None, None, "lat", "lon"),
            P("lat", "lon"),
            P("lat", "lon"),
            P("lat", "lon"),
        ),
        out_specs=(P(None, "lat", "lon"), P(None, None, None, ("lat", "lon"))),
        check_vma=False,
    )
```

```python
import functools
import math

import jax
import jax.numpy as jnp
from jax import lax
from jax.experimental import pallas as pl
from jax.experimental.pallas import tpu as pltpu
from jax.sharding import PartitionSpec as P

BASINS = 10
MESH = pl.DeviceIdType.MESH
SUB = 8
LANES = 128


def kernel(
    lat_devices, lon_devices, snapshots, levels, share_rows,
    flow_hbm, warmth_hbm, flag_hbm, floor_hbm, label_hbm,
    eddy_ref, transport_ref,
    flag_ref, floor_ref, label_ref, depth, flow, warmth, average, dots,
    halo_out, halo_in, stats, received, sums, pair_sums, chip_sums, peer_sums, peer_last,
    load_flow, load_warmth, load_columns, halo_send, halo_recv,
    stat_send, stat_recv, pair_send, pair_recv, sum_send, sum_recv, last_send, last_recv,
):
    rows = flow.shape[1]
    blocks = rows // SUB
    last = blocks - 1
    owners = SUB // share_rows
    planes = snapshots * levels
    packed = stats.shape[1]
    fields = dots.shape[0] // SUB
    used = BASINS * SUB
    lat = lax.axis_index("lat")
    me = lax.axis_index("lon")
    own_block = me // owners
    scaling = 1.0 / math.sqrt(LANES * lon_devices)

    def window(b):
        return pl.ds(pl.multiple_of(b * SUB, SUB), SUB)

    def flow_copy(b):
        at = window(b)
        return pltpu.make_async_copy(flow_hbm.at[:, at, :], flow.at[:, at, :], load_flow.at[b])

    def warmth_copy(b):
        at = window(b)
        return pltpu.make_async_copy(warmth_hbm.at[:, at, :], warmth.at[:, at, :], load_warmth.at[b])

    columns = [
        pltpu.make_async_copy(src, dst, load_columns.at[n])
        for n, (src, dst) in enumerate(
            ((flag_hbm, flag_ref), (floor_hbm, floor_ref), (label_hbm, label_ref))
        )
    ]
    for copy in columns:
        copy.start()
    for b in range(blocks):
        warmth_copy(b).start()
        flow_copy(b).start()

    barrier = pltpu.get_barrier_semaphore()

    def greet(d, carry):
        pl.semaphore_signal(
            barrier, inc=1, device_id=(lat, lax.rem(me + d, lon_devices)), device_id_type=MESH
        )
        return carry

    @pl.when(lat > 0)
    def _():
        pl.semaphore_signal(barrier, inc=1, device_id=(lat - 1, me), device_id_type=MESH)

    @pl.when(lat < lat_devices - 1)
    def _():
        pl.semaphore_signal(barrier, inc=1, device_id=(lat + 1, me), device_id_type=MESH)

    lax.fori_loop(1, lon_devices, greet, 0)

    halo_copy = pltpu.make_async_remote_copy(
        src_ref=halo_out, dst_ref=halo_in, send_sem=halo_send, recv_sem=halo_recv,
        device_id=(jnp.maximum(lat - 1, 0), me), device_id_type=MESH,
    )

    chips = lon_devices // 2
    core = lax.rem(me, 2)
    pair_copy = pltpu.make_async_remote_copy(
        src_ref=sums.at[pl.ds(0, last)], dst_ref=pair_sums, send_sem=pair_send, recv_sem=pair_recv,
        device_id=(lat, me + 1 - 2 * core), device_id_type=MESH,
    )

    def chip_copy(to, source):
        return pltpu.make_async_remote_copy(
            src_ref=chip_sums, dst_ref=peer_sums.at[source],
            send_sem=sum_send.at[to], recv_sem=sum_recv.at[source],
            device_id=(lat, 2 * to + core), device_id_type=MESH,
        )

    def last_copy(to, source):
        return pltpu.make_async_remote_copy(
            src_ref=sums.at[last], dst_ref=peer_last.at[source],
            send_sem=last_send.at[to], recv_sem=last_recv.at[source],
            device_id=(lat, to), device_id_type=MESH,
        )

    def each_chip(action):
        def step(d, carry):
            action(lax.rem(me // 2 + d, chips))
            return carry

        lax.fori_loop(1, chips, step, 0)

    def stat_copy(b, to, source):
        return pltpu.make_async_remote_copy(
            src_ref=stats.at[b], dst_ref=received.at[source],
            send_sem=stat_send.at[to], recv_sem=stat_recv.at[source],
            device_id=(lat, to), device_id_type=MESH,
        )

    def each_peer(action):
        def step(d, carry):
            action(lax.rem(me + d, lon_devices))
            return carry

        lax.fori_loop(1, lon_devices, step, 0)

    sub = lax.broadcasted_iota(jnp.int32, (SUB, LANES), 0)
    level = lax.broadcasted_iota(jnp.int32, (levels, SUB, LANES), 0).astype(jnp.float32)

    def next_row(here, after):
        first = lax.broadcasted_iota(jnp.int32, here.shape, here.ndim - 2) == 0
        return pltpu.roll(jnp.where(first, after, here), SUB - 1, here.ndim - 2)

    def both_halves(x):
        return x + pltpu.roll(x, levels, 0)

    def wet_cells(b):
        here = depth[window(b), :]
        limit = jnp.minimum(here, next_row(here, depth[window(b + 1), :]))
        return (level < limit[None]).astype(jnp.float32)

    def block_stats(b, carry):
        at = window(b)
        wet = wet_cells(b)
        velocity = flow[:, at, :].reshape(snapshots, levels, SUB, LANES)
        here = warmth[:, at, :]
        point = (0.5 * (here + next_row(here, warmth[:, window(b + 1), :]))).reshape(
            snapshots, levels, SUB, LANES
        )
        mean_velocity = jnp.sum(velocity, axis=0) * (1.0 / snapshots)
        mean_warmth = jnp.sum(point, axis=0) * (1.0 / snapshots)
        cross = jnp.sum((velocity - mean_velocity) * (point - mean_warmth), axis=0) * (1.0 / snapshots)
        average[:, at, :] = mean_warmth
        values = jnp.concatenate(
            [
                (velocity * wet[None]).reshape(planes, SUB, LANES),
                (point * wet[None]).reshape(planes, SUB, LANES),
                wet,
                wet,
                mean_velocity * mean_warmth * wet,
                cross * wet,
            ],
            axis=0,
        ).reshape(-1, LANES)
        high = values.astype(jnp.bfloat16)
        low = (values - high.astype(jnp.float32)).astype(jnp.bfloat16)
        labels = label_ref[at, :]
        member = jnp.concatenate(
            [(labels == n).astype(jnp.float32) for n in range(LANES // SUB)], axis=0
        ).astype(jnp.bfloat16)
        dots[...] = lax.dot_general(
            jnp.concatenate([high, low], axis=1), jnp.concatenate([member, member], axis=1),
            (((1,), (1,)), ((), ())), preferred_element_type=jnp.float32,
        )
        row_of = lax.rem(lax.broadcasted_iota(jnp.int32, (fields, LANES), 1), SUB)
        zonal = dots[pl.ds(0, fields, stride=SUB), :]
        for j in range(1, SUB):
            zonal = jnp.where(row_of == j, dots[pl.ds(j, fields, stride=SUB), :], zonal)
        warmth_sum = both_halves(
            jnp.sum(zonal[planes : 2 * planes].reshape(planes // SUB, SUB, LANES), axis=0)
        )
        count = zonal[2 * planes : 2 * planes + SUB]
        sums[pl.ds(b, 1)] = jnp.where(sub < levels, warmth_sum, count)[None]
        half = packed // 2
        rest = zonal[packed:]
        spare = lax.broadcasted_iota(jnp.int32, (half, LANES), 1) >= used
        stats[pl.ds(b, 1)] = jnp.concatenate(
            [
                jnp.where(spare, pltpu.roll(rest, used, 1), zonal[:half]),
                jnp.where(spare, pltpu.roll(rest, 2 * used - LANES, 1), zonal[half:packed]),
            ],
            axis=0,
        )[None]
        return carry

    for copy in columns:
        copy.wait()
    depth[pl.ds(0, rows), :] = (flag_ref[...] * floor_ref[...]).astype(jnp.float32)
    for b in range(blocks):
        warmth_copy(b).wait()
    halo_out[pl.ds(0, planes), :] = warmth[:, 0, :]
    halo_out[pl.ds(planes, SUB), :] = depth[pl.ds(0, SUB), :]

    def early_block(b, carry):
        flow_copy(b).wait()
        return block_stats(b, carry)

    lax.fori_loop(0, last // 2, early_block, 0)

    pl.semaphore_wait(
        barrier,
        lon_devices - 1 + (lat > 0).astype(jnp.int32) + (lat < lat_devices - 1).astype(jnp.int32),
    )

    @pl.when(lat > 0)
    def _():
        halo_copy.start()

    lax.fori_loop(last // 2, last, early_block, 0)
    pair_copy.start()

    def send_stats(to):
        @pl.when(to // owners < last)
        def _():
            stat_copy(to // owners, to, me).start()

    each_peer(send_stats)
    pair_copy.wait_recv()
    chip_sums[...] = sums[pl.ds(0, last)] + pair_sums[...]
    each_chip(lambda to: chip_copy(to, me // 2).start())
    flow_copy(last).wait()

    @pl.when(lat < lat_devices - 1)
    def _():
        halo_copy.wait_recv()
        warmth[:, rows, :] = halo_in[pl.ds(0, planes), :]
        depth[pl.ds(rows, SUB), :] = halo_in[pl.ds(planes, SUB), :]

    @pl.when(lat == lat_devices - 1)
    def _():
        warmth[:, rows, :] = jnp.zeros((planes, LANES), jnp.float32)
        depth[pl.ds(rows, SUB), :] = jnp.zeros((SUB, LANES), jnp.float32)

    block_stats(last, 0)
    each_peer(lambda to: last_copy(to, me).start())

    def send_last(to):
        @pl.when(to // owners == last)
        def _():
            stat_copy(last, to, me).start()

    each_peer(send_last)

    def block_eddy(b, block_sums):
        at = pl.ds(b * SUB, SUB)
        wet = wet_cells(b)
        index = label_ref[at, :] * SUB + sub
        bar = block_sums / jnp.maximum(pltpu.roll(block_sums, levels, 0), 1.0) * (1.0 / snapshots)
        for k in range(levels):
            cells = jnp.take_along_axis(
                jnp.broadcast_to(bar[k : k + 1], (SUB, LANES)), index, axis=1
            )
            eddy_ref[k, at, :] = wet[k] * (average[k, at, :] - cells)

    def add_sums(d, total):
        source = lax.rem(me // 2 + chips - d, chips)
        chip_copy(0, source).wait_recv()
        return total + peer_sums[pl.ds(source, 1)][0]

    first_sums = lax.fori_loop(1, chips, add_sums, chip_sums[...])
    for b in range(last):
        block_eddy(b, first_sums[b])

    def add_received(d, total):
        source = lax.rem(me + lon_devices - d, lon_devices)
        stat_copy(0, me, source).wait_recv()
        return total + received[pl.ds(source, 1)][0]

    total = lax.fori_loop(1, lon_devices, add_received, stats[pl.ds(own_block, 1)][0])
    half = packed // 2
    lane = lax.broadcasted_iota(jnp.int32, (half, LANES), 1)
    total = jnp.concatenate(
        [
            total,
            jnp.where(
                lane < LANES - used,
                pltpu.roll(total[:half], LANES - used, 1),
                pltpu.roll(total[half:], 2 * LANES - 2 * used, 1),
            ),
        ],
        axis=0,
    )
    count = total[2 * planes : 2 * planes + SUB]
    divisor = jnp.maximum(count, 1.0)
    means_v = total[:planes].reshape(planes // SUB, SUB, LANES) / divisor
    means_t = total[planes : 2 * planes].reshape(planes // SUB, SUB, LANES) / divisor
    bar_v = both_halves(jnp.sum(means_v, axis=0)) * (1.0 / snapshots)
    bar_t = both_halves(jnp.sum(means_t, axis=0)) * (1.0 / snapshots)
    swing = both_halves(jnp.sum((means_v - bar_v) * (means_t - bar_t), axis=0)) * (1.0 / snapshots)
    upper = jnp.where(sub < levels, scaling * count * bar_v * bar_t, scaling * count * swing)
    lower = scaling * total[2 * planes + SUB : 2 * planes + 2 * SUB] - upper
    if owners > 1:
        shift = LANES - lax.rem(me, owners) * share_rows
        upper = pltpu.roll(upper, shift, 1)
        lower = pltpu.roll(lower, shift, 1)
    spread = lax.rem(lax.broadcasted_iota(jnp.int32, (SUB, LANES), 1) * SUB + sub, LANES)
    for c, part in enumerate((upper, lower, upper, lower)):
        for k in range(levels):
            row = c // 2 * levels + k
            table = jnp.take_along_axis(
                jnp.broadcast_to(part[row : row + 1], (SUB, LANES)), spread, axis=1
            )
            transport_ref[c, k] = table[:share_rows, :BASINS]

    def add_last(d, total):
        source = lax.rem(me + lon_devices - d, lon_devices)
        last_copy(0, source).wait_recv()
        return total + peer_last[pl.ds(source, 1)][0]

    block_eddy(last, lax.fori_loop(1, lon_devices, add_last, sums[last]))

    @pl.when(lat > 0)
    def _():
        halo_copy.wait_send()

    pair_copy.wait_send()
    each_chip(lambda to: chip_copy(to, me // 2).wait_send())

    def sent(to):
        last_copy(to, me).wait_send()
        stat_copy(to // owners, to, me).wait_send()

    each_peer(sent)


def shards(
    lat_devices, lon_devices,
    poleward_flow, potential_warmth, water_profile_flag, floor_count, catchment_label_for_site,
):
    snapshots, levels, rows, columns = poleward_flow.shape
    share_rows = rows // lon_devices
    blocks = rows // SUB
    planes = snapshots * levels
    fields = 2 * planes + 4 * levels
    packed = fields * 2 // 3
    f32, i32, vmem, dma = jnp.float32, jnp.int32, pltpu.VMEM, pltpu.SemaphoreType.DMA
    eddy_temp, transport = pl.pallas_call(
        functools.partial(kernel, lat_devices, lon_devices, snapshots, levels, share_rows),
        out_shape=(
            vmem((levels, rows, columns), f32),
            vmem((4, levels, share_rows, BASINS), f32),
        ),
        in_specs=[pl.BlockSpec(memory_space=pltpu.HBM)] * 5,
        out_specs=(pl.BlockSpec(memory_space=vmem), pl.BlockSpec(memory_space=vmem)),
        scratch_shapes=[
            vmem((rows, columns), i32),
            vmem((rows, columns), i32),
            vmem((rows, columns), i32),
            vmem((rows + SUB, columns), f32),
            vmem((planes, rows, columns), f32),
            vmem((planes, rows + SUB, columns), f32),
            vmem((levels, rows, columns), f32),
            vmem((fields * SUB, LANES), f32),
            vmem((planes + SUB, LANES), f32),
            vmem((planes + SUB, LANES), f32),
            vmem((blocks, packed, LANES), f32),
            vmem((lon_devices, packed, LANES), f32),
            vmem((blocks, SUB, LANES), f32),
            vmem((blocks - 1, SUB, LANES), f32),
            vmem((blocks - 1, SUB, LANES), f32),
            vmem((lon_devices // 2, blocks - 1, SUB, LANES), f32),
            vmem((lon_devices, SUB, LANES), f32),
            dma((blocks,)),
            dma((blocks,)),
            dma((3,)),
            dma,
            dma,
            dma((lon_devices,)),
            dma((lon_devices,)),
            dma,
            dma,
            dma((lon_devices // 2,)),
            dma((lon_devices // 2,)),
            dma((lon_devices,)),
            dma((lon_devices,)),
        ],
        compiler_params=pltpu.CompilerParams(
            collective_id=0, has_side_effects=True, vmem_limit_bytes=62 * 1024 * 1024
        ),
        name="heat_transport",
    )(
        poleward_flow.reshape(planes, rows, columns),
        potential_warmth.reshape(planes, rows, columns),
        water_profile_flag,
        floor_count,
        catchment_label_for_site,
    )
    return eddy_temp, jnp.transpose(transport, (0, 3, 1, 2))


def solution(mesh):
    return jax.shard_map(
        functools.partial(shards, mesh.shape["lat"], mesh.shape["lon"]),
        mesh=mesh,
        in_specs=(
            P(None, None, "lat", "lon"),
            P(None, None, "lat", "lon"),
            P("lat", "lon"),
            P("lat", "lon"),
            P("lat", "lon"),
        ),
        out_specs=(P(None, "lat", "lon"), P(None, None, None, ("lat", "lon"))),
        check_vma=False,
    )
```

```python
import functools
import math

import jax
import jax.numpy as jnp
from jax import lax
from jax.experimental import pallas as pl
from jax.experimental.pallas import tpu as pltpu
from jax.sharding import PartitionSpec as P

BASINS = 10
MESH = pl.DeviceIdType.MESH
SUB = 8
LANES = 128


def kernel(
    lat_devices, lon_devices, snapshots, levels, share_rows,
    flow_hbm, warmth_hbm, flag_hbm, floor_hbm, label_hbm,
    eddy_ref, transport_ref,
    flag_ref, floor_ref, label_ref, depth, flow, warmth, average, dots,
    halo_out, halo_in, stats, received, sums, pair_sums, chip_sums, peer_sums, peer_last,
    load_flow, load_warmth, load_columns, halo_send, halo_recv,
    stat_send, stat_recv, pair_send, pair_recv, sum_send, sum_recv, last_send, last_recv,
):
    rows = flow.shape[1]
    blocks = rows // SUB
    last = blocks - 1
    owners = SUB // share_rows
    planes = snapshots * levels
    packed = stats.shape[1]
    fields = dots.shape[1] // SUB
    used = BASINS * SUB
    lat = lax.axis_index("lat")
    me = lax.axis_index("lon")
    own_block = me // owners
    scaling = 1.0 / math.sqrt(LANES * lon_devices)

    def window(b):
        return pl.ds(pl.multiple_of(b * SUB, SUB), SUB)

    def flow_copy(b):
        at = window(b)
        return pltpu.make_async_copy(flow_hbm.at[:, at, :], flow.at[:, at, :], load_flow.at[b])

    def warmth_copy(b):
        at = window(b)
        return pltpu.make_async_copy(warmth_hbm.at[:, at, :], warmth.at[:, at, :], load_warmth.at[b])

    columns = [
        pltpu.make_async_copy(src, dst, load_columns.at[n])
        for n, (src, dst) in enumerate(
            ((flag_hbm, flag_ref), (floor_hbm, floor_ref), (label_hbm, label_ref))
        )
    ]
    for copy in columns:
        copy.start()
    for b in range(blocks):
        warmth_copy(b).start()
        flow_copy(b).start()

    barrier = pltpu.get_barrier_semaphore()

    def greet(d, carry):
        pl.semaphore_signal(
            barrier, inc=1, device_id=(lat, lax.rem(me + d, lon_devices)), device_id_type=MESH
        )
        return carry

    @pl.when(lat > 0)
    def _():
        pl.semaphore_signal(barrier, inc=1, device_id=(lat - 1, me), device_id_type=MESH)

    @pl.when(lat < lat_devices - 1)
    def _():
        pl.semaphore_signal(barrier, inc=1, device_id=(lat + 1, me), device_id_type=MESH)

    lax.fori_loop(1, lon_devices, greet, 0)

    halo_copy = pltpu.make_async_remote_copy(
        src_ref=halo_out, dst_ref=halo_in, send_sem=halo_send, recv_sem=halo_recv,
        device_id=(jnp.maximum(lat - 1, 0), me), device_id_type=MESH,
    )

    chips = lon_devices // 2
    core = lax.rem(me, 2)
    pair_copy = pltpu.make_async_remote_copy(
        src_ref=sums.at[pl.ds(0, last)], dst_ref=pair_sums, send_sem=pair_send, recv_sem=pair_recv,
        device_id=(lat, me + 1 - 2 * core), device_id_type=MESH,
    )

    def chip_copy(to, source):
        return pltpu.make_async_remote_copy(
            src_ref=chip_sums, dst_ref=peer_sums.at[source],
            send_sem=sum_send.at[to], recv_sem=sum_recv.at[source],
            device_id=(lat, 2 * to + core), device_id_type=MESH,
        )

    def last_copy(to, source):
        return pltpu.make_async_remote_copy(
            src_ref=sums.at[last], dst_ref=peer_last.at[source],
            send_sem=last_send.at[to], recv_sem=last_recv.at[source],
            device_id=(lat, to), device_id_type=MESH,
        )

    def each_chip(action):
        def step(d, carry):
            action(lax.rem(me // 2 + d, chips))
            return carry

        lax.fori_loop(1, chips, step, 0)

    def stat_copy(b, to, source):
        return pltpu.make_async_remote_copy(
            src_ref=stats.at[b], dst_ref=received.at[source],
            send_sem=stat_send.at[to], recv_sem=stat_recv.at[source],
            device_id=(lat, to), device_id_type=MESH,
        )

    def each_peer(action):
        def step(d, carry):
            action(lax.rem(me + d, lon_devices))
            return carry

        lax.fori_loop(1, lon_devices, step, 0)

    sub = lax.broadcasted_iota(jnp.int32, (SUB, LANES), 0)
    level = lax.broadcasted_iota(jnp.int32, (levels, SUB, LANES), 0).astype(jnp.float32)

    def next_row(here, after):
        first = lax.broadcasted_iota(jnp.int32, here.shape, here.ndim - 2) == 0
        return pltpu.roll(jnp.where(first, after, here), SUB - 1, here.ndim - 2)

    def both_halves(x):
        return x + pltpu.roll(x, levels, 0)

    def wet_cells(b):
        here = depth[window(b), :]
        limit = jnp.minimum(here, next_row(here, depth[window(b + 1), :]))
        return (level < limit[None]).astype(jnp.float32)

    def block_stats(b, carry):
        at = window(b)
        wet = wet_cells(b)
        velocity = flow[:, at, :].reshape(snapshots, levels, SUB, LANES)
        here = warmth[:, at, :]
        point = (0.5 * (here + next_row(here, warmth[:, window(b + 1), :]))).reshape(
            snapshots, levels, SUB, LANES
        )
        mean_velocity = jnp.sum(velocity, axis=0) * (1.0 / snapshots)
        mean_warmth = jnp.sum(point, axis=0) * (1.0 / snapshots)
        cross = jnp.sum((velocity - mean_velocity) * (point - mean_warmth), axis=0) * (1.0 / snapshots)
        average[:, at, :] = mean_warmth
        values = jnp.concatenate(
            [
                (velocity * wet[None]).reshape(planes, SUB, LANES),
                (point * wet[None]).reshape(planes, SUB, LANES),
                wet,
                wet,
                mean_velocity * mean_warmth * wet,
                cross * wet,
            ],
            axis=0,
        ).reshape(-1, LANES)
        high = values.astype(jnp.bfloat16)
        low = (values - high.astype(jnp.float32)).astype(jnp.bfloat16)
        labels = label_ref[at, :]
        member = jnp.concatenate(
            [(labels == n).astype(jnp.float32) for n in range(LANES // SUB)], axis=0
        ).astype(jnp.bfloat16)
        dots[b] = lax.dot_general(
            jnp.concatenate([high, low], axis=1), jnp.concatenate([member, member], axis=1),
            (((1,), (1,)), ((), ())), preferred_element_type=jnp.float32,
        )
        row_of = lax.rem(lax.broadcasted_iota(jnp.int32, (fields, LANES), 1), SUB)
        zonal = dots[b, pl.ds(0, fields, stride=SUB), :]
        for j in range(1, SUB):
            zonal = jnp.where(row_of == j, dots[b, pl.ds(j, fields, stride=SUB), :], zonal)
        warmth_sum = both_halves(
            jnp.sum(zonal[planes : 2 * planes].reshape(planes // SUB, SUB, LANES), axis=0)
        )
        count = zonal[2 * planes : 2 * planes + SUB]
        sums[pl.ds(b, 1)] = jnp.where(sub < levels, warmth_sum, count)[None]
        half = packed // 2
        rest = zonal[packed:]
        spare = lax.broadcasted_iota(jnp.int32, (half, LANES), 1) >= used
        stats[pl.ds(b, 1)] = jnp.concatenate(
            [
                jnp.where(spare, pltpu.roll(rest, used, 1), zonal[:half]),
                jnp.where(spare, pltpu.roll(rest, 2 * used - LANES, 1), zonal[half:packed]),
            ],
            axis=0,
        )[None]
        return carry

    for copy in columns:
        copy.wait()
    depth[pl.ds(0, rows), :] = (flag_ref[...] * floor_ref[...]).astype(jnp.float32)
    for b in range(blocks):
        warmth_copy(b).wait()
    halo_out[pl.ds(0, planes), :] = warmth[:, 0, :]
    halo_out[pl.ds(planes, SUB), :] = depth[pl.ds(0, SUB), :]

    def early_block(b, carry):
        flow_copy(b).wait()
        return block_stats(b, carry)

    for b in range(blocks):
        flow_copy(b).wait()
    for b in range(last // 2):
        block_stats(b, 0)

    pl.semaphore_wait(
        barrier,
        lon_devices - 1 + (lat > 0).astype(jnp.int32) + (lat < lat_devices - 1).astype(jnp.int32),
    )

    @pl.when(lat > 0)
    def _():
        halo_copy.start()

    for b in range(last // 2, last):
        block_stats(b, 0)
    pair_copy.start()

    def send_stats(to):
        @pl.when(to // owners < last)
        def _():
            stat_copy(to // owners, to, me).start()

    each_peer(send_stats)
    pair_copy.wait_recv()
    chip_sums[...] = sums[pl.ds(0, last)] + pair_sums[...]
    each_chip(lambda to: chip_copy(to, me // 2).start())

    @pl.when(lat < lat_devices - 1)
    def _():
        halo_copy.wait_recv()
        warmth[:, rows, :] = halo_in[pl.ds(0, planes), :]
        depth[pl.ds(rows, SUB), :] = halo_in[pl.ds(planes, SUB), :]

    @pl.when(lat == lat_devices - 1)
    def _():
        warmth[:, rows, :] = jnp.zeros((planes, LANES), jnp.float32)
        depth[pl.ds(rows, SUB), :] = jnp.zeros((SUB, LANES), jnp.float32)

    block_stats(last, 0)
    each_peer(lambda to: last_copy(to, me).start())

    def send_last(to):
        @pl.when(to // owners == last)
        def _():
            stat_copy(last, to, me).start()

    each_peer(send_last)

    def block_eddy(b, block_sums):
        at = pl.ds(b * SUB, SUB)
        wet = wet_cells(b)
        index = label_ref[at, :] * SUB + sub
        bar = block_sums / jnp.maximum(pltpu.roll(block_sums, levels, 0), 1.0) * (1.0 / snapshots)
        for k in range(levels):
            cells = jnp.take_along_axis(
                jnp.broadcast_to(bar[k : k + 1], (SUB, LANES)), index, axis=1
            )
            eddy_ref[k, at, :] = wet[k] * (average[k, at, :] - cells)

    def add_sums(d, total):
        source = lax.rem(me // 2 + chips - d, chips)
        chip_copy(0, source).wait_recv()
        return total + peer_sums[pl.ds(source, 1)][0]

    first_sums = lax.fori_loop(1, chips, add_sums, chip_sums[...])
    for b in range(last):
        block_eddy(b, first_sums[b])

    def add_received(d, total):
        source = lax.rem(me + lon_devices - d, lon_devices)
        stat_copy(0, me, source).wait_recv()
        return total + received[pl.ds(source, 1)][0]

    total = lax.fori_loop(1, lon_devices, add_received, stats[pl.ds(own_block, 1)][0])
    half = packed // 2
    lane = lax.broadcasted_iota(jnp.int32, (half, LANES), 1)
    total = jnp.concatenate(
        [
            total,
            jnp.where(
                lane < LANES - used,
                pltpu.roll(total[:half], LANES - used, 1),
                pltpu.roll(total[half:], 2 * LANES - 2 * used, 1),
            ),
        ],
        axis=0,
    )
    count = total[2 * planes : 2 * planes + SUB]
    divisor = jnp.maximum(count, 1.0)
    means_v = total[:planes].reshape(planes // SUB, SUB, LANES) / divisor
    means_t = total[planes : 2 * planes].reshape(planes // SUB, SUB, LANES) / divisor
    bar_v = both_halves(jnp.sum(means_v, axis=0)) * (1.0 / snapshots)
    bar_t = both_halves(jnp.sum(means_t, axis=0)) * (1.0 / snapshots)
    swing = both_halves(jnp.sum((means_v - bar_v) * (means_t - bar_t), axis=0)) * (1.0 / snapshots)
    upper = jnp.where(sub < levels, scaling * count * bar_v * bar_t, scaling * count * swing)
    lower = scaling * total[2 * planes + SUB : 2 * planes + 2 * SUB] - upper
    if owners > 1:
        shift = LANES - lax.rem(me, owners) * share_rows
        upper = pltpu.roll(upper, shift, 1)
        lower = pltpu.roll(lower, shift, 1)
    spread = lax.rem(lax.broadcasted_iota(jnp.int32, (SUB, LANES), 1) * SUB + sub, LANES)
    for c, part in enumerate((upper, lower, upper, lower)):
        for k in range(levels):
            row = c // 2 * levels + k
            table = jnp.take_along_axis(
                jnp.broadcast_to(part[row : row + 1], (SUB, LANES)), spread, axis=1
            )
            transport_ref[c, k] = table[:share_rows, :BASINS]

    def add_last(d, total):
        source = lax.rem(me + lon_devices - d, lon_devices)
        last_copy(0, source).wait_recv()
        return total + peer_last[pl.ds(source, 1)][0]

    block_eddy(last, lax.fori_loop(1, lon_devices, add_last, sums[last]))

    @pl.when(lat > 0)
    def _():
        halo_copy.wait_send()

    pair_copy.wait_send()
    each_chip(lambda to: chip_copy(to, me // 2).wait_send())

    def sent(to):
        last_copy(to, me).wait_send()
        stat_copy(to // owners, to, me).wait_send()

    each_peer(sent)


def shards(
    lat_devices, lon_devices,
    poleward_flow, potential_warmth, water_profile_flag, floor_count, catchment_label_for_site,
):
    snapshots, levels, rows, columns = poleward_flow.shape
    share_rows = rows // lon_devices
    blocks = rows // SUB
    planes = snapshots * levels
    fields = 2 * planes + 4 * levels
    packed = fields * 2 // 3
    f32, i32, vmem, dma = jnp.float32, jnp.int32, pltpu.VMEM, pltpu.SemaphoreType.DMA
    eddy_temp, transport = pl.pallas_call(
        functools.partial(kernel, lat_devices, lon_devices, snapshots, levels, share_rows),
        out_shape=(
            vmem((levels, rows, columns), f32),
            vmem((4, levels, share_rows, BASINS), f32),
        ),
        in_specs=[pl.BlockSpec(memory_space=pltpu.HBM)] * 5,
        out_specs=(pl.BlockSpec(memory_space=vmem), pl.BlockSpec(memory_space=vmem)),
        scratch_shapes=[
            vmem((rows, columns), i32),
            vmem((rows, columns), i32),
            vmem((rows, columns), i32),
            vmem((rows + SUB, columns), f32),
            vmem((planes, rows, columns), f32),
            vmem((planes, rows + SUB, columns), f32),
            vmem((levels, rows, columns), f32),
            vmem((blocks, fields * SUB, LANES), f32),
            vmem((planes + SUB, LANES), f32),
            vmem((planes + SUB, LANES), f32),
            vmem((blocks, packed, LANES), f32),
            vmem((lon_devices, packed, LANES), f32),
            vmem((blocks, SUB, LANES), f32),
            vmem((blocks - 1, SUB, LANES), f32),
            vmem((blocks - 1, SUB, LANES), f32),
            vmem((lon_devices // 2, blocks - 1, SUB, LANES), f32),
            vmem((lon_devices, SUB, LANES), f32),
            dma((blocks,)),
            dma((blocks,)),
            dma((3,)),
            dma,
            dma,
            dma((lon_devices,)),
            dma((lon_devices,)),
            dma,
            dma,
            dma((lon_devices // 2,)),
            dma((lon_devices // 2,)),
            dma((lon_devices,)),
            dma((lon_devices,)),
        ],
        compiler_params=pltpu.CompilerParams(
            collective_id=0, has_side_effects=True, vmem_limit_bytes=62 * 1024 * 1024
        ),
        name="heat_transport",
    )(
        poleward_flow.reshape(planes, rows, columns),
        potential_warmth.reshape(planes, rows, columns),
        water_profile_flag,
        floor_count,
        catchment_label_for_site,
    )
    return eddy_temp, jnp.transpose(transport, (0, 3, 1, 2))


def solution(mesh):
    return jax.shard_map(
        functools.partial(shards, mesh.shape["lat"], mesh.shape["lon"]),
        mesh=mesh,
        in_specs=(
            P(None, None, "lat", "lon"),
            P(None, None, "lat", "lon"),
            P("lat", "lon"),
            P("lat", "lon"),
            P("lat", "lon"),
        ),
        out_specs=(P(None, "lat", "lon"), P(None, None, None, ("lat", "lon"))),
        check_vma=False,
    )
```
